32 devices in a mesh: dp: 8 (over y, x, core), tensor: 4 (over z).
Axes of the slice: x: 2, y: 2, z: 4, core: 2. Of those that a mesh axis runs over, the one named last changes fastest.
Arguments:
- features: bfloat16 [2048, 1024], P(('dp', 'tensor')), may hold values from -6 to 6
- click: int32 [2048], P(('dp', 'tensor')), may hold values 0 or 1
- convert: int32 [2048], P(('dp', 'tensor')), may hold values 0 or 1
- w1: bfloat16 [1024, 2, 4096], P('dp', None, 'tensor'), may hold values from -0.1875 to 0.1875
- b1: float32 [2, 4096], P(None, 'tensor'), may hold values from -4 to 4
- w2: bfloat16 [2, 4096], P(None, 'tensor'), may hold values from -0.1875 to 0.1875
Outputs:
- sample_loss: float32 [2048], P(('dp', 'tensor'))
- grad_features: bfloat16 [2048, 1024], P(('dp', 'tensor'))
- grad_w1: float32 [1024, 2, 4096], P('dp', None, 'tensor')
- grad_b1: float32 [2, 4096], P(None, 'tensor')
- grad_w2: float32 [2, 4096], P(None, 'tensor')
The draws below stay inside these ranges and needn't reach their ends.
All inputs are finite; a program needn't handle non-finite values. No bound on the sum of `click` or of `convert` on one device may be relied on, other than what follows from the above.
Results may differ from the reference program's by a relative error of at most 0.025.
Values may be sent and summed in bfloat16 or wider, within the bound.
No kernel may reach another device: no remote copies, remote signals or barrier semaphores. Data moves between devices by JAX's collectives and lax.ppermute only.
A program may use at most 64 MiB of HBM per device.

```python
import math
import jax
import jax.numpy as jnp
from jax import lax

D = 1024
H = 4096
SAMPLES = 2048


def plant(array, own_key, low, top_value):
    dims = array.shape
    place = [jax.random.randint(jax.random.fold_in(own_key, axis), (), 0, dims[axis]) for axis in range(len(dims))]
    array = array.at[tuple(place)].set(low)
    longest = dims.index(max(dims))
    place[longest] = (place[longest] + 1) % dims[longest]
    return array.at[tuple(place)].set(top_value)


def spiked(entries, own_key, source, target, shards_of, factor):
    owner, partner = [(jnp.arange(entries.shape[position]) // (entries.shape[position] // shards_of)).reshape([-1 if axis == position else 1 for axis in range(entries.ndim)]) for position in (source, target)]
    chosen = jax.random.permutation(own_key, shards_of)[partner]
    strong = (owner == chosen) | (owner == (partner + shards_of // 2) % shards_of)
    return jnp.where(strong, factor * entries, entries)


def block_scale(stream_key, extent, pieces, least, top_value):
    factor_of, own = 1.0, jax.random.fold_in(stream_key, 6)
    for dim, parts in pieces:
        heights = jnp.exp(jax.random.uniform(jax.random.fold_in(own, dim), (parts,), jnp.float32, least / len(pieces), top_value / len(pieces)))
        factor_of = factor_of * jnp.repeat(heights, extent[dim] // parts).reshape([-1 if axis == dim else 1 for axis in range(len(extent))])
    return factor_of


def normal_values(stream_key, dims, scale, most, cuts=(), held_as=jnp.bfloat16):
    drawn = jax.random.normal(stream_key, dims, jnp.float32) * scale
    if len(cuts) > 0:
        drawn = block_scale(stream_key, dims, cuts, -0.22, 0.18) * drawn
    return jnp.clip(drawn, min=-most, max=most).astype(held_as)


def bell_draw_with(key, extent, scale, bound, cuts, heavy, held_as=jnp.bfloat16):
    values = scale * jax.random.normal(key, extent, jnp.float32)
    if cuts:
        values = values * block_scale(key, extent, cuts, -0.22, 0.18)
    return jnp.clip(spiked(values, jax.random.fold_in(key, 3), *heavy), -bound, bound).astype(held_as)


def setup_inputs(seed: int = 0) -> dict:
    key_list = jax.random.split(jax.random.key(seed), 7)
    features = bell_draw_with(key_list[0], (SAMPLES, D), 1.0, 6.0, ((0, 32),), (0, 1, 32, 2.75))
    click = plant((jax.random.randint(key_list[1], (SAMPLES,), 0, 3) < 1).astype(jnp.int32), jax.random.fold_in(key_list[1], 1), 0, 1)
    convert = plant((jax.random.randint(key_list[2], (SAMPLES,), 0, 2) < 1).astype(jnp.int32), jax.random.fold_in(key_list[2], 1), 0, 1)
    w1 = normal_values(key_list[3], (D, 2, H), D ** -0.5, 0.1875, ((0, 8), (2, 4)))
    b1 = normal_values(key_list[4], (2, H), 0.7, 4.0, ((1, 4),), jnp.float32)
    w2 = normal_values(key_list[5], (2, H), (H // 4) ** -0.5, 0.1875, ((1, 4),))
    return {"features": features, "click": click, "convert": convert, "w1": w1, "b1": b1, "w2": w2}


def sample_loss_fn(logits, click, convert):
    first = logits[:, 0]
    second = logits[:, 1]
    label_y = click.astype(jnp.float32)
    label_z = (click * convert).astype(jnp.float32)
    rest = jnp.log(jax.nn.sigmoid(-first) + jax.nn.sigmoid(first) * jax.nn.sigmoid(-second))
    click_part = label_y * jax.nn.log_sigmoid(first) + (1.0 - label_y) * jax.nn.log_sigmoid(-first)
    both_part = label_z * (jax.nn.log_sigmoid(first) + jax.nn.log_sigmoid(second)) + (1.0 - label_z) * rest
    return -click_part - both_part

def reference(features, click, convert, w1, b1, w2):
    total, width = features.shape
    hidden_units = w1.shape[2]
    block = min(total, 4096)
    blocks = total // block
    w_flat = w1.reshape(width, 2 * hidden_units)
    w2f = w2.astype(jnp.float32)

    def step(carry, inputs):
        acc_w1, acc_b1, acc_w2 = carry
        rows, clicks, converts = inputs
        pre = jnp.dot(rows, w_flat, preferred_element_type=jnp.float32).reshape(block, 2, hidden_units) + b1[None]
        hidden = jnp.maximum(pre, 0.0).astype(jnp.bfloat16)
        logits = lax.optimization_barrier(jnp.sum(hidden.astype(jnp.float32) * w2f[None], axis=2))
        losses, pullback = jax.vjp(lambda value: sample_loss_fn(value, clicks, converts), logits)
        slope = pullback(jnp.ones_like(losses))[0]
        dhidden = jnp.where(pre > 0.0, slope[:, :, None] * w2f[None], 0.0).astype(jnp.bfloat16)
        d_flat = dhidden.reshape(block, 2 * hidden_units)
        grad_rows = jnp.dot(d_flat, w_flat.T, preferred_element_type=jnp.float32).astype(jnp.bfloat16)
        acc_w1 = acc_w1 + jnp.dot(rows.T, d_flat, preferred_element_type=jnp.float32).reshape(width, 2, hidden_units)
        acc_b1 = acc_b1 + lax.optimization_barrier(jnp.sum(dhidden.astype(jnp.float32), axis=0))
        acc_w2 = acc_w2 + lax.optimization_barrier(jnp.sum(slope[:, :, None] * hidden.astype(jnp.float32), axis=0))
        return ((acc_w1, acc_b1, acc_w2), (losses, grad_rows))
    start = (jnp.zeros((width, 2, hidden_units), jnp.float32), jnp.zeros((2, hidden_units), jnp.float32), jnp.zeros((2, hidden_units), jnp.float32))
    carry, outs = lax.scan(step, start, (features.reshape(blocks, block, width), click.reshape(blocks, block), convert.reshape(blocks, block)))
    scale = 1.0 / math.sqrt(total)
    losses = outs[0].reshape(total)
    grad_features = outs[1].reshape(total, width)
    return (losses, grad_features, carry[0] * scale, carry[1] * scale, carry[2] * scale)
```

```python
import math

import jax
import jax.numpy as jnp
from jax import lax
from jax.sharding import PartitionSpec as P

AXES = ("dp", "tensor")
BF = jnp.bfloat16
F32 = jnp.float32


def sample_loss_fn(logits, click, convert):
    first = logits[:, 0]
    second = logits[:, 1]
    label_y = click.astype(jnp.float32)
    label_z = (click * convert).astype(jnp.float32)
    rest = jnp.log(jax.nn.sigmoid(-first) + jax.nn.sigmoid(first) * jax.nn.sigmoid(-second))
    click_part = label_y * jax.nn.log_sigmoid(first) + (1.0 - label_y) * jax.nn.log_sigmoid(-first)
    both_part = (
        label_z * (jax.nn.log_sigmoid(first) + jax.nn.log_sigmoid(second)) + (1.0 - label_z) * rest
    )
    return -click_part - both_part


def loss_slope(logits, click, convert):
    losses, pullback = jax.vjp(lambda value: sample_loss_fn(value, click, convert), logits)
    return (losses, pullback(jnp.ones_like(losses))[0])


def general(features, click, convert, w1, b1, w2):
    own_count, width = features.shape
    local_units = w1.shape[2]
    total = own_count * lax.axis_size("dp") * lax.axis_size("tensor")
    scale = 1.0 / math.sqrt(total)
    group = lax.all_gather(features, "tensor", axis=0, tiled=True)
    group_count = group.shape[0]
    w2f = w2.astype(jnp.float32)
    full_weights = lax.all_gather(w1, "dp", axis=0, tiled=True)
    w_flat = full_weights.reshape(width, 2 * local_units)
    pre_flat = jnp.dot(group, w_flat, preferred_element_type=jnp.float32)
    pre = pre_flat.reshape(group_count, 2, local_units) + b1[None]
    hidden = jnp.maximum(pre, 0.0).astype(jnp.bfloat16)
    partial_logits = jnp.sum(hidden.astype(jnp.float32) * w2f[None], axis=2)
    logits = lax.psum(partial_logits, "tensor")
    labels = lax.all_gather(jnp.stack([click, convert], axis=1), "tensor", axis=0, tiled=True)
    losses_all, slope = loss_slope(logits, labels[:, 0], labels[:, 1])
    offset = lax.axis_index("tensor") * own_count
    losses = lax.dynamic_slice_in_dim(losses_all, offset, own_count, 0)
    dhidden = jnp.where(pre > 0.0, slope[:, :, None] * w2f[None], 0.0).astype(jnp.bfloat16)
    d_flat = dhidden.reshape(group_count, 2 * local_units)
    partial_rows = jnp.dot(d_flat, w_flat.T, preferred_element_type=jnp.float32)
    grad_features = lax.psum_scatter(
        partial_rows.astype(jnp.bfloat16), "tensor", scatter_dimension=0, tiled=True
    )
    partial_w1 = jnp.dot(group.T, d_flat, preferred_element_type=jnp.float32)
    grad_w1 = (
        lax.psum_scatter(
            partial_w1.reshape(width, 2, local_units), "dp", scatter_dimension=0, tiled=True
        )
        * scale
    )
    bias_term = jnp.sum(dhidden.astype(jnp.float32), axis=0)
    out_term = jnp.sum(slope[:, :, None] * hidden.astype(jnp.float32), axis=0)
    summed = lax.psum(jnp.concatenate([bias_term, out_term], axis=0), "dp")
    return (losses, grad_features, grad_w1, summed[0:2] * scale, summed[2:4] * scale)


def send(value, mask, tensor_size, dp_size):
    pairs = [
        (d * tensor_size + t, (d ^ mask[0]) * tensor_size + (t ^ mask[1]))
        for d in range(dp_size)
        for t in range(tensor_size)
    ]
    return lax.ppermute(value, AXES, pairs)


def split_pair(value):
    high = value.astype(BF)
    return (high, (value - high.astype(F32)).astype(BF))


def cube(features, click, convert, w1, b1, w2):
    own, width = features.shape
    rows, towers, units = w1.shape
    n_dp, n_t = lax.axis_size("dp"), lax.axis_size("tensor")
    half = units // 2
    scale = 1.0 / math.sqrt(own * n_dp * n_t)
    ex = lambda value, *mask: send(value, mask, n_t, n_dp)
    CORE, X, Y = 1, 2, 4
    me = lax.axis_index("dp")
    core = me % 2
    chip = me // 2

    def half_of(which):
        return lax.dynamic_slice_in_dim(w1, which * half, half, 2).reshape(rows, towers * half)

    mine, other = half_of(core), half_of(1 - core)
    lab_y = click.astype(BF)
    lab_z = (click * convert).astype(BF)
    aug = jnp.concatenate(
        [features, jnp.pad(jnp.stack([lab_y, lab_z], axis=1), ((0, 0), (0, 126)))], axis=1
    )

    x_other = ex(other, X | CORE, 0)
    y_mine = ex(mine, Y, 0)
    x_mine = ex(mine, X, 0)
    y_other = ex(other, Y | CORE, 0)
    sib = ex(other, CORE, 0)
    zs = [ex(aug, 0, k) for k in range(n_t - 1, 0, -1)][::-1]
    core_samples = jnp.concatenate([aug] + zs, axis=0)
    d_mine = ex(y_mine, X, 0)
    d_other = ex(x_other, Y, 0)
    sib_samples = ex(core_samples, CORE, 0)
    samples = jnp.concatenate([core_samples, sib_samples], axis=0)
    count = samples.shape[0]

    def columns(block):
        start = ((chip ^ block) * 2 + core) * rows
        start_sib = ((chip ^ block) * 2 + 1 - core) * rows
        return jnp.concatenate(
            [
                lax.dynamic_slice_in_dim(samples, start, rows, 1),
                lax.dynamic_slice_in_dim(samples, start_sib, rows, 1),
            ],
            axis=1,
        )

    feats = [columns(b) for b in range(4)]
    weights = [
        jnp.concatenate(pair, axis=0)
        for pair in ((mine, sib), (x_mine, x_other), (y_mine, y_other), (d_mine, d_other))
    ]
    bias = lax.dynamic_slice_in_dim(b1, core * half, half, 1).reshape(1, towers * half)
    outw = lax.dynamic_slice_in_dim(w2, core * half, half, 1).astype(F32)

    pre = jnp.dot(jnp.concatenate(feats, 1), jnp.concatenate(weights, 0), preferred_element_type=F32)
    pre = pre + bias
    hidden = jnp.maximum(pre, 0.0).astype(BF)
    part = hidden.astype(F32) * outw.reshape(1, towers * half)
    logits = jnp.sum(part.reshape(count, towers, half), axis=2).T

    def reorder(value, core_bit, k):
        blocks = value.reshape(towers, 2, n_t, own)
        if core_bit:
            blocks = blocks[:, ::-1]
        order = [j ^ k for j in range(n_t)]
        return jnp.concatenate([blocks[:, :, j : j + 1] for j in order], axis=2).reshape(towers, count)

    logits = logits + reorder(ex(logits, CORE, 0), True, 0)
    step = 1
    while step < n_t:
        logits = logits + reorder(ex(logits, 0, step), False, step)
        step *= 2
    logits = logits.T
    y_all = samples[:, width].astype(F32)
    z_all = samples[:, width + 1].astype(F32)
    losses_all, slope = loss_slope(logits, y_all, z_all)
    losses = losses_all[:own]

    slope_w = jnp.concatenate(
        [slope[:, t : t + 1] * outw[t : t + 1, :] for t in range(towers)], axis=1
    )
    dhidden = jnp.where(pre > 0.0, slope_w, 0.0).astype(BF)
    d_t = [dhidden[:, t * half : (t + 1) * half] for t in range(towers)]

    def piece(block, t):
        return jnp.dot(feats[block].T, d_t[t], preferred_element_type=F32)

    bias_sum = [jnp.sum(d.astype(F32), axis=0) for d in d_t]
    out_sum = [
        jnp.sum(slope[:, t : t + 1] * hidden[:, t * half : (t + 1) * half].astype(F32), axis=0)
        for t in range(towers)
    ]
    vectors = [jnp.stack([bias_sum[t], out_sum[t]]) for t in range(towers)]

    def packed(main, vector):
        high, low = split_pair(vector)
        tail = jnp.pad(jnp.concatenate([high, low], axis=0), ((0, 12), (0, 0)))
        return jnp.concatenate([main.astype(BF), tail], axis=0)

    def unpacked(value):
        main, tail = value[: 2 * rows].astype(F32), value[2 * rows :].astype(F32)
        return main, tail[0:2] + tail[2:4]

    finals = []
    for t, (first, second, via_first, via_second) in enumerate(((X, Y, 1, 2), (Y, X, 2, 1))):
        far = ex(packed(piece(3, t), vectors[t]), first, 0)
        near = ex(piece(via_first, t).astype(BF), first, 0)
        far_main, far_vec = unpacked(far)
        vec = vectors[t] + far_vec
        relay = ex(packed(piece(via_second, t) + far_main, vec), second, 0)
        relay_main, relay_vec = unpacked(relay)
        finals.append((piece(0, t) + near.astype(F32) + relay_main, vec + relay_vec))

    back = []
    for t, (main, vec) in enumerate(finals):
        high, low = split_pair(vec)
        back.append(
            ex(
                jnp.concatenate(
                    [main[rows:].astype(BF), high, low, jnp.zeros((12, half), BF)], axis=0
                ),
                CORE,
                0,
            )
        )
    halves = []
    for t, (main, vec) in enumerate(finals):
        got = back[t].astype(F32)
        got_vec = got[rows : rows + 2] + got[rows + 2 : rows + 4]
        low_half = lambda a, b: jnp.concatenate(
            [jnp.where(core == 0, a, b), jnp.where(core == 0, b, a)], axis=-1
        )
        halves.append((low_half(main[:rows], got[:rows]) * scale, low_half(vec, got_vec) * scale))
    grad_w1 = jnp.stack([h[0] for h in halves], axis=1)
    grad_b1 = jnp.stack([h[1][0] for h in halves], axis=0)
    grad_w2 = jnp.stack([h[1][1] for h in halves], axis=0)

    stacked = jnp.concatenate(weights, 0)
    partial_rows = jnp.dot(dhidden, stacked.T, preferred_element_type=F32)
    keep, give = partial_rows[: count // 2], partial_rows[count // 2 :]
    def placed(value):
        parts = [None] * 8
        out = jnp.zeros((value.shape[0], width), value.dtype)
        for b in range(4):
            for s in range(2):
                start = ((chip ^ b) * 2 + (core ^ s)) * rows
                block = value[:, (2 * b + s) * rows : (2 * b + s + 1) * rows]
                out = lax.dynamic_update_slice_in_dim(out, block, start, 1)
        return out

    keep = placed(keep) + ex(placed(give).astype(BF), CORE, 0).astype(F32)
    blocks = [keep[k * own : (k + 1) * own] for k in range(n_t)]
    grad_features = blocks[0]
    for k in range(1, n_t):
        grad_features = grad_features + ex(blocks[k].astype(BF), 0, k).astype(F32)
    return (losses, grad_features.astype(BF), grad_w1, grad_b1, grad_w2)


def power_of_two(n):
    return n & (n - 1) == 0


def solution(mesh):
    placed = (
        P(("dp", "tensor"), None),
        P(("dp", "tensor")),
        P(("dp", "tensor")),
        P("dp", None, "tensor"),
        P(None, "tensor"),
        P(None, "tensor"),
    )
    local = cube if mesh.shape["dp"] == 8 and power_of_two(mesh.shape["tensor"]) else general
    return jax.shard_map(
        local,
        mesh=mesh,
        in_specs=placed,
        out_specs=(
            P(("dp", "tensor")),
            P(("dp", "tensor"), None),
            P("dp", None, "tensor"),
            P(None, "tensor"),
            P(None, "tensor"),
        ),
        check_vma=False,
    )
```

```python
import math

import jax
import jax.numpy as jnp
from jax import lax
from jax.experimental import pallas as pl
from jax.experimental.pallas import tpu as pltpu
from jax.sharding import PartitionSpec as P

AXES = ("dp", "tensor")
BF = jnp.bfloat16
F32 = jnp.float32


def sample_loss_fn(logits, click, convert):
    first = logits[:, 0]
    second = logits[:, 1]
    label_y = click.astype(jnp.float32)
    label_z = (click * convert).astype(jnp.float32)
    rest = jnp.log(jax.nn.sigmoid(-first) + jax.nn.sigmoid(first) * jax.nn.sigmoid(-second))
    click_part = label_y * jax.nn.log_sigmoid(first) + (1.0 - label_y) * jax.nn.log_sigmoid(-first)
    both_part = (
        label_z * (jax.nn.log_sigmoid(first) + jax.nn.log_sigmoid(second)) + (1.0 - label_z) * rest
    )
    return -click_part - both_part


def loss_slope(logits, click, convert):
    losses, pullback = jax.vjp(lambda value: sample_loss_fn(value, click, convert), logits)
    return (losses, pullback(jnp.ones_like(losses))[0])


def general(features, click, convert, w1, b1, w2):
    own_count, width = features.shape
    local_units = w1.shape[2]
    total = own_count * lax.axis_size("dp") * lax.axis_size("tensor")
    scale = 1.0 / math.sqrt(total)
    group = lax.all_gather(features, "tensor", axis=0, tiled=True)
    group_count = group.shape[0]
    w2f = w2.astype(jnp.float32)
    full_weights = lax.all_gather(w1, "dp", axis=0, tiled=True)
    w_flat = full_weights.reshape(width, 2 * local_units)
    pre_flat = jnp.dot(group, w_flat, preferred_element_type=jnp.float32)
    pre = pre_flat.reshape(group_count, 2, local_units) + b1[None]
    hidden = jnp.maximum(pre, 0.0).astype(jnp.bfloat16)
    partial_logits = jnp.sum(hidden.astype(jnp.float32) * w2f[None], axis=2)
    logits = lax.psum(partial_logits, "tensor")
    labels = lax.all_gather(jnp.stack([click, convert], axis=1), "tensor", axis=0, tiled=True)
    losses_all, slope = loss_slope(logits, labels[:, 0], labels[:, 1])
    offset = lax.axis_index("tensor") * own_count
    losses = lax.dynamic_slice_in_dim(losses_all, offset, own_count, 0)
    dhidden = jnp.where(pre > 0.0, slope[:, :, None] * w2f[None], 0.0).astype(jnp.bfloat16)
    d_flat = dhidden.reshape(group_count, 2 * local_units)
    partial_rows = jnp.dot(d_flat, w_flat.T, preferred_element_type=jnp.float32)
    grad_features = lax.psum_scatter(
        partial_rows.astype(jnp.bfloat16), "tensor", scatter_dimension=0, tiled=True
    )
    partial_w1 = jnp.dot(group.T, d_flat, preferred_element_type=jnp.float32)
    grad_w1 = (
        lax.psum_scatter(
            partial_w1.reshape(width, 2, local_units), "dp", scatter_dimension=0, tiled=True
        )
        * scale
    )
    bias_term = jnp.sum(dhidden.astype(jnp.float32), axis=0)
    out_term = jnp.sum(slope[:, :, None] * hidden.astype(jnp.float32), axis=0)
    summed = lax.psum(jnp.concatenate([bias_term, out_term], axis=0), "dp")
    return (losses, grad_features, grad_w1, summed[0:2] * scale, summed[2:4] * scale)


def send(value, mask, tensor_size, dp_size):
    pairs = [
        (d * tensor_size + t, (d ^ mask[0]) * tensor_size + (t ^ mask[1]))
        for d in range(dp_size)
        for t in range(tensor_size)
    ]
    return lax.ppermute(value, AXES, pairs)


def call(body, outs, args, flops=0, nbytes=0, vmem=16):
    spec = pl.BlockSpec(memory_space=pltpu.VMEM)
    return pl.pallas_call(
        body,
        out_shape=[jax.ShapeDtypeStruct(shape, dtype) for shape, dtype in outs],
        in_specs=[spec] * len(args),
        out_specs=[spec] * len(outs),
        compiler_params=pltpu.CompilerParams(vmem_limit_bytes=vmem << 20),
        cost_estimate=pl.CostEstimate(
            flops=max(int(flops), 1 << 20), bytes_accessed=int(nbytes), transcendentals=0
        ),
    )(*args)


def place():
    me = lax.axis_index("dp")
    return (lax.div(me, 2), lax.rem(me, 2), lax.axis_index("tensor"))


def at(index, size):
    return pl.ds(pl.multiple_of(index * size, size), size)


def mm(a, b):
    return jnp.dot(a, b, preferred_element_type=F32)


def mm_t(a, b):
    return lax.dot_general(a, b, (((1,), (1,)), ((), ())), preferred_element_type=F32)


def with_tail(vec):
    return jnp.concatenate([vec, vec - vec.astype(BF).astype(F32)], axis=0).astype(BF)


def from_tail(tail):
    tail = tail.astype(F32)
    return tail[:8] + tail[8:]


def join_body(n_t, own, *refs):
    blocks, out = refs[:n_t], refs[n_t]
    _, _, z = place()
    row = lax.broadcasted_iota(jnp.int32, (16, out.shape[1]), 0)
    labels = jnp.zeros((16, out.shape[1]), F32)
    for k in range(n_t):
        where = z ^ k
        out[at(where, own), :] = blocks[k][:own, :]
        line = jnp.broadcast_to(blocks[k][own : own + 16, :].astype(F32)[0:1, :], labels.shape)
        labels = jnp.where(row == where, line, labels)
    out[n_t * own :, :] = labels.astype(BF)


def turn_body(count, pair, mine, theirs, x, lab, *turned):
    chip, core, _ = place()
    half = count // 2
    x[at(core, half), :] = mine[:half, :]
    x[at(1 - core, half), :] = theirs[:half, :]
    lab[at(core, 16), :] = mine[half:, :].astype(F32)
    lab[at(1 - core, 16), :] = theirs[half:, :].astype(F32)
    for b in range(4):
        turned[b][...] = x[:, at(chip ^ b, pair)].astype(F32).T.astype(BF)


def first_body(pair, x, m0, o0, m1, o1, m2, o2, acc, w_0, w_1, w_2):
    chip, core, _ = place()
    rows = pair // 2
    for w, m, o in ((w_0, m0, o0), (w_1, m1, o1), (w_2, m2, o2)):
        w[at(core, rows), :] = m[...]
        w[at(1 - core, rows), :] = o[...]
    acc[...] = mm(x[:, at(chip, pair)], w_0[...])
    acc[...] += mm(x[:, at(chip ^ 1, pair)], w_1[...])
    acc[...] += mm(x[:, at(chip ^ 2, pair)], w_2[...])


def last_body(pair, acc, x, m3, o3, bias, out_rows, hidden, logits, w_3):
    chip, core, _ = place()
    rows = pair // 2
    w_3[at(core, rows), :] = m3[...]
    w_3[at(1 - core, rows), :] = o3[...]
    pre = acc[...] + mm(x[:, at(chip ^ 3, pair)], w_3[...]) + bias[...]
    hidden[...] = jnp.maximum(pre, 0.0).astype(BF)
    logits[...] = mm_t(out_rows[...], hidden[...])[:8]


def gate_body(hidden, out_rows, gated):
    line = jnp.sum(out_rows[...].astype(F32), axis=0, keepdims=True)
    gated[...] = jnp.where(hidden[...].astype(F32) > 0.0, line, 0.0).astype(BF)


def add_body(a, b, out):
    out[...] = a[...] + b[...]


def slope_body(half, pair, a, b, labels, gated, hidden, xt, losses, dh, vec, far0, far1):
    total = a[...] + b[...]
    first, second = total[0:1], total[1:2]
    y, z = labels[0:1], labels[1:2]
    s_a, s_b = jax.nn.sigmoid(first), jax.nn.sigmoid(second)
    n_a, n_b = jax.nn.sigmoid(-first), jax.nn.sigmoid(-second)
    rest = n_a + s_a * n_b
    log_a, log_b = jax.nn.log_sigmoid(first), jax.nn.log_sigmoid(second)
    log_na = jax.nn.log_sigmoid(-first)
    losses[...] = -(y * log_a + (1.0 - y) * log_na) - (
        z * (log_a + log_b) + (1.0 - z) * jnp.log(rest)
    )
    share = (1.0 - z) / rest
    slope_a = (s_a - y) - (z * n_a - share * (s_a * n_a * s_b))
    slope_b = -(z * n_b - share * (s_a * s_b * n_b))
    count = total.shape[1]
    slopes = jnp.concatenate([slope_a, slope_b, jnp.zeros((6, count), F32)], axis=0)
    column = slopes.T
    for t in range(2):
        cols = slice(t * half, (t + 1) * half)
        dh[:, cols] = (column[:, t : t + 1] * gated[:, cols].astype(F32)).astype(BF)
    for t, far in ((0, far0), (1, far1)):
        far[: pair, :] = mm(xt[...], dh[:, t * half : (t + 1) * half]).astype(BF)
    bias = mm(jnp.ones((16, count), BF), dh[...])
    out = mm(with_tail(slopes), hidden[...])
    out = out[:8] + out[8:]
    row = lax.broadcasted_iota(jnp.int32, (8, half), 0)
    for t, far in ((0, far0), (1, far1)):
        cols = slice(t * half, (t + 1) * half)
        own = jnp.where(
            row == 0, bias[:8, cols], jnp.broadcast_to(out[t : t + 1, cols], (8, half))
        )
        vec[:, cols] = own
        far[pair:, :] = with_tail(own)


def near_body(half, dh, xt1, xt2, near0, near1):
    near0[...] = mm(xt1[...], dh[:, :half]).astype(BF)
    near1[...] = mm(xt2[...], dh[:, half:]).astype(BF)


def own_body(half, dh, xt0, xt1, xt2, relay0, relay1, own0, own1):
    relay0[...] = mm(xt2[...], dh[:, :half])
    relay1[...] = mm(xt1[...], dh[:, half:])
    own0[...] = mm(xt0[...], dh[:, :half])
    own1[...] = mm(xt0[...], dh[:, half:])


def relay_body(pair, base, vec, got, out, vec_out):
    out[:pair, :] = (base[...] + got[:pair, :].astype(F32)).astype(BF)
    total = vec[...] + from_tail(got[pair:, :])
    vec_out[...] = total
    out[pair:, :] = with_tail(total)


def final_body(pair, base, near, got, vec, keep, give, vec_out):
    _, core, _ = place()
    rows = pair // 2
    total = vec[...] + from_tail(got[pair:, :])
    vec_out[...] = total
    give[rows:, :] = with_tail(total)
    for which, away in ((core, False), (1 - core, True)):
        part = at(which, rows)
        value = base[part, :] + near[part, :].astype(F32) + got[part, :].astype(F32)
        if away:
            give[:rows, :] = value.astype(BF)
        else:
            keep[...] = value


def out_body(half, scale, keep0, keep1, got0, got1, vec0, vec1, grad_w1, grad_b1, grad_w2):
    _, core, _ = place()
    rows = keep0.shape[0]
    here, there = at(core, half), at(1 - core, half)
    for t, (keep, got, vec) in enumerate(((keep0, got0, vec0), (keep1, got1, vec1))):
        grad_w1[:, t, here] = keep[...] * scale
        grad_w1[:, t, there] = got[:rows, :].astype(F32) * scale
        other = from_tail(got[rows:, :]) * scale
        mine = vec[...] * scale
        for row, grad in ((0, grad_b1), (1, grad_w2)):
            grad[t : t + 1, here] = mine[row : row + 1]
            grad[t : t + 1, there] = other[row : row + 1]


def back_body(pair, dh, w_0, w_1, w_2, w_3, keep, give):
    chip, core, _ = place()
    half = dh.shape[0] // 2
    for b, w in enumerate((w_0, w_1, w_2, w_3)):
        give[:, at(chip ^ b, pair)] = mm_t(dh[at(1 - core, half), :], w[...]).astype(BF)
    for b, w in enumerate((w_0, w_1, w_2, w_3)):
        keep[:, at(chip ^ b, pair)] = mm_t(dh[at(core, half), :], w[...])


def spread_body(n_t, own, keep, got, *outs):
    _, _, z = place()
    for k in range(n_t):
        part = at(z ^ k, own)
        value = keep[part, :] + got[part, :].astype(F32)
        outs[k][...] = value.astype(outs[k].dtype)


def sum_body(*refs):
    total = refs[0][...]
    for ref in refs[1:-1]:
        total = total + ref[...].astype(F32)
    refs[-1][...] = total.astype(refs[-1].dtype)


def cube(features, click, convert, w1, b1, w2):
    own, width = features.shape
    rows, towers, units = w1.shape
    n_dp, n_t = lax.axis_size("dp"), lax.axis_size("tensor")
    half = units // 2
    cols = towers * half
    pair = 2 * rows
    count = 2 * n_t * own
    scale = 1.0 / math.sqrt(own * n_dp * n_t)
    CORE, X, Y = 1, 2, 4
    _, core, z = place()

    def ex(value, mask):
        return send(value, mask, n_t, n_dp)

    def part(fn, *static):
        return lambda *refs: fn(*static, *refs)

    def half_of(which):
        return lax.dynamic_slice_in_dim(w1, which * half, half, 2).reshape(rows, cols)

    mine, other = half_of(core), half_of(1 - core)
    label = jnp.concatenate(
        [
            jnp.pad(click.astype(BF), (0, 128 - own)),
            jnp.pad((click * convert).astype(BF), (0, width - 128 - own)),
        ]
    )
    aug = jnp.concatenate([features, jnp.pad(label[None], ((0, 15), (0, 0)))], axis=0)

    x_other = ex(other, (X | CORE, 0))
    y_mine = ex(mine, (Y, 0))
    x_mine = ex(mine, (X, 0))
    y_other = ex(other, (Y | CORE, 0))
    sib = ex(other, (CORE, 0))
    zs = [ex(aug, (0, k)) for k in range(1, n_t)]
    d_mine = ex(y_mine, (X, 0))
    d_other = ex(x_other, (Y, 0))
    (core_samples,) = call(part(join_body, n_t, own), [((n_t * own + 16, width), BF)], [aug] + zs)
    sib_samples = ex(core_samples, (CORE, 0))
    x, lab, xt0, xt1, xt2, xt3 = call(
        part(turn_body, count, pair),
        [((count, width), BF), ((32, width), F32)] + [((pair, count), BF)] * 4,
        [core_samples, sib_samples],
    )
    lab = lab.reshape(2, 16, width)
    labels = jnp.stack(
        [lab[:, :n_t, :own].reshape(count), lab[:, :n_t, 128 : 128 + own].reshape(count)]
    )
    bias = lax.dynamic_slice_in_dim(b1, core * half, half, 1).reshape(1, cols)
    w2_half = lax.dynamic_slice_in_dim(w2, core * half, half, 1)
    out_rows = jnp.concatenate(
        [
            jnp.pad(w2_half[t : t + 1], ((0, 0), (t * half, cols - (t + 1) * half)))
            for t in range(towers)
        ]
        + [jnp.zeros((14, cols), BF)],
        axis=0,
    )

    acc, w_0, w_1, w_2 = call(
        part(first_body, pair),
        [((count, cols), F32)] + [((pair, cols), BF)] * 3,
        [x, mine, sib, x_mine, x_other, y_mine, y_other],
        flops=6 * count * pair * cols,
    )
    hidden, logits, w_3 = call(
        part(last_body, pair),
        [((count, cols), BF), ((8, count), F32), ((pair, cols), BF)],
        [acc, x, d_mine, d_other, bias, out_rows],
        flops=2 * count * pair * cols,
    )
    (gated,) = call(gate_body, [((count, cols), BF)], [hidden, out_rows], flops=1 << 29)

    def step(a, b):
        return call(add_body, [((8, count), F32)], [a, b])[0]

    got = ex(logits, (CORE, 0))
    k = 1
    while k < n_t:
        logits = step(logits, got)
        got = ex(logits, (0, k))
        k *= 2
    losses_all, dh, vec, far0, far1 = call(
        part(slope_body, half, pair),
        [((1, count), F32), ((count, cols), BF), ((8, cols), F32)]
        + [((pair + 16, half), BF)] * 2,
        [logits, got, labels, gated, hidden, xt3],
        flops=6 * count * pair * cols,
    )
    losses = lax.dynamic_slice_in_dim(losses_all[0], (core * n_t + z) * own, own, 0)

    far0 = ex(far0, (X, 0))
    far1 = ex(far1, (Y, 0))
    near0, near1 = call(
        part(near_body, half),
        [((pair, half), BF)] * 2,
        [dh, xt1, xt2],
        flops=2 * count * pair * cols,
    )
    near0 = ex(near0, (X, 0))
    near1 = ex(near1, (Y, 0))
    base0, base1, own0, own1 = call(
        part(own_body, half),
        [((pair, half), F32)] * 4,
        [dh, xt0, xt1, xt2],
        flops=4 * count * pair * cols,
    )
    keep, give = call(
        part(back_body, pair),
        [((count // 2, width), F32), ((count // 2, width), BF)],
        [dh, w_0, w_1, w_2, w_3],
        flops=2 * count * width * cols,
    )
    got = ex(give, (CORE, 0))
    blocks = call(
        part(spread_body, n_t, own),
        [((own, width), F32)] + [((own, width), BF)] * (n_t - 1),
        [keep, got],
    )
    row_parts = [ex(blocks[k], (0, k)) for k in range(1, n_t)]
    (grad_features,) = call(sum_body, [((own, width), BF)], [blocks[0]] + row_parts)

    kept = []
    for t, base, mine_t, far, near, via in (
        (0, base0, own0, far0, near0, Y),
        (1, base1, own1, far1, near1, X),
    ):
        vec_t = vec[:, t * half : (t + 1) * half]
        relay, vec_t = call(
            part(relay_body, pair), [((pair + 16, half), BF), ((8, half), F32)], [base, vec_t, far]
        )
        relay = ex(relay, (via, 0))
        kept.append(
            call(
                part(final_body, pair),
                [((rows, half), F32), ((rows + 16, half), BF), ((8, half), F32)],
                [mine_t, near, relay, vec_t],
            )
        )
    backs = [ex(kept[t][1], (CORE, 0)) for t in range(towers)]
    grad_w1, grad_b1, grad_w2 = call(
        part(out_body, half, scale),
        [((rows, towers, units), F32), ((towers, units), F32), ((towers, units), F32)],
        [kept[0][0], kept[1][0], backs[0], backs[1], kept[0][2], kept[1][2]],
    )
    return (losses, grad_features, grad_w1, grad_b1, grad_w2)


def power_of_two(n):
    return n & (n - 1) == 0


def solution(mesh):
    placed = (
        P(("dp", "tensor"), None),
        P(("dp", "tensor")),
        P(("dp", "tensor")),
        P("dp", None, "tensor"),
        P(None, "tensor"),
        P(None, "tensor"),
    )
    local = cube if mesh.shape["dp"] == 8 and power_of_two(mesh.shape["tensor"]) else general
    return jax.shard_map(
        local,
        mesh=mesh,
        in_specs=placed,
        out_specs=(
            P(("dp", "tensor")),
            P(("dp", "tensor"), None),
            P("dp", None, "tensor"),
            P(None, "tensor"),
            P(None, "tensor"),
        ),
        check_vma=False,
    )
```
